32 devices in a mesh: kpt: 4 (over y, x), pw: 8 (over z, core).
Axes of the slice: x: 2, y: 2, z: 4, core: 2. Of those that a mesh axis runs over, the one named last changes fastest.
Arguments:
- energies: float32 [16, 512], P('kpt', 'pw'), may hold values from 0.5 to 3
- current: float32 [2, 16, 512], P(None, 'kpt', 'pw'), may hold values from -40 to 40
- previous: float32 [2, 16, 512], P(None, 'kpt', 'pw'), may hold values from -6 to 6
- previous_beta: float32 [2], replicated, may hold values from 0.5 to 2
- pair_left: bfloat16 [16, 512, 4096], P('kpt', None, 'pw'), may hold values from -0.09375 to 0.09375
- pair_right: bfloat16 [16, 512, 4096], P('kpt', None, 'pw'), may hold values from -0.25 to 0.25
- screened: bfloat16 [16, 4096, 4096], P('kpt', 'pw'), may hold values from -0.0234375 to 0.0234375
- momentum_index: int32 [16, 16], replicated, may hold values from 0 to 15, each once within a row
Outputs:
- last_vector: float32 [2, 16, 512], P(None, 'kpt', 'pw')
- prior_vector: float32 [2, 16, 512], P(None, 'kpt', 'pw')
- alpha_terms: float32 [2, 3], replicated
- beta_terms: float32 [2, 3], replicated
The draws below stay inside these ranges and needn't reach their ends.
Inputs may be any that keep to these rules, and one draw needn't show every extreme that they name: Each row of momentum_index names every index from 0 to 15 once.
All inputs are finite; a program needn't handle non-finite values.
Results may differ from the reference program's by a relative error of at most 0.003.
Values may be sent and summed in bfloat16 or wider, within the bound.
A program may use at most 128 MiB of HBM per device.

```python
import math
import jax
import jax.numpy as jnp
from jax import lax

NK = 16
NC = 512
NG = 4096
NVEC = 2
STEPS = 3


def draw_current(key, part):
    normal_part = jnp.clip(jax.random.normal(key, (NVEC, NK, NC), jnp.float32), -4.0, 4.0)
    kpoint_frac = jnp.arange(NK, dtype=jnp.float32) / NK
    band_frac = jnp.arange(NC, dtype=jnp.float32) / NC
    values = normal_part
    kpoint_scale = 10.0 ** (kpoint_frac - 0.5)
    band_scale = 10.0 ** (band_frac - 0.5)
    return values * kpoint_scale[None, :, None] * band_scale[None, None, :]


def block_scale(stream_key, shape, pieces, smallest, high):
    def one(axis_at, blocks):
        steps = jax.random.uniform(jax.random.fold_in(jax.random.fold_in(stream_key, 6), axis_at), (blocks,), jnp.float32, smallest / len(pieces), high / len(pieces))
        return jnp.repeat(jnp.exp(steps), shape[axis_at] // blocks).reshape((-1,) + (1,) * (len(shape) - axis_at - 1))

    factor_of = one(*pieces[0])
    for cut in pieces[1:]:
        factor_of = factor_of * one(*cut)
    return factor_of


def centred(stream_key, dims, scale, reach, cuts=(), held_as=jnp.bfloat16):
    values = jax.random.normal(stream_key, dims, jnp.float32) * scale
    if len(cuts) > 0:
        values = block_scale(stream_key, dims, cuts, -0.22, 0.18) * values
    return jnp.clip(values, min=-reach, max=reach).astype(held_as)


def setup_inputs(seed: int = 0) -> dict:
    key_list = jax.random.split(jax.random.key(seed), 9)
    energies = jnp.clip(0.5 + 2.5 * jax.random.uniform(key_list[0], (NK, NC), jnp.float32) ** block_scale(key_list[0], (NK, NC), ((0, 4), (1, 8)), -0.2, 0.2), 0.5, 3.0)
    current = draw_current(jax.random.fold_in(key_list[8], 71), 0)
    previous = centred(key_list[2], (NVEC, NK, NC), 1.0, 6.0, ((1, 4), (2, 8)), jnp.float32)
    previous_beta = jnp.clip(jnp.exp(jax.random.uniform(key_list[3], (NVEC,), jnp.float32, math.log(0.5), math.log(2.0))), 0.5, 2.0)
    pair_left = centred(key_list[4], (NK, NC, NG), NG ** -0.5, 0.09375, ((0, 4), (2, 8)))
    pair_right = centred(key_list[5], (NK, NC, NG), NC ** -0.5, 0.25, ((0, 4), (2, 8)))
    screened = centred(key_list[6], (NK, NG, NG), (NK * NG) ** -0.5, 0.0234375, ((0, 4), (1, 8)))
    momentum_index = jax.vmap(lambda own: jax.random.permutation(own, NK))(jax.random.split(key_list[7], NK)).reshape((NK, NK)).astype(jnp.int32)
    return dict(energies=energies, current=current, previous=previous, previous_beta=previous_beta, pair_left=pair_left, pair_right=pair_right, screened=screened, momentum_index=momentum_index)


epsilon = 1e-06

def reference(energies, current, previous, previous_beta, pair_left, pair_right, screened, momentum_index):
    entries = NK * NC
    left_float = pair_left.astype(jnp.float32)
    right_float = pair_right.astype(jnp.float32)
    vector = current
    earlier = previous
    beta_before = previous_beta
    alpha_list = []
    beta_list = []
    for turn_index in range(STEPS):
        rounded = vector.astype(jnp.bfloat16)
        density = jnp.einsum('kcg,vkc->kvg', right_float, rounded.astype(jnp.float32), precision=lax.Precision.HIGHEST).astype(jnp.bfloat16)
        columns = density.reshape(NK * NVEC, NG).T

        def add_transfer(running, qpoint):
            images = jnp.dot(screened[qpoint], columns, preferred_element_type=jnp.float32).reshape(NG, NK, NVEC)
            selector = (momentum_index == qpoint).astype(jnp.float32)
            return (running + jnp.einsum('jk,gkv->jvg', selector, images, precision=lax.Precision.HIGHEST), None)
        potential, unused = lax.scan(add_transfer, jnp.zeros((NK, NVEC, NG), jnp.float32), jnp.arange(NK, dtype=jnp.int32))
        potential_bf = potential.astype(jnp.bfloat16)
        direct = jnp.einsum('kcg,kvg->vkc', left_float, potential_bf.astype(jnp.float32), precision=lax.Precision.HIGHEST)
        applied = energies[None] * vector - direct - beta_before[:, None, None] * earlier
        alpha_now = lax.optimization_barrier(jnp.sum(vector * applied, axis=(1, 2))) / entries
        residual = applied - alpha_now[:, None, None] * vector
        beta_now = jnp.sqrt(lax.optimization_barrier(jnp.sum(residual * residual, axis=(1, 2))) / entries + epsilon)
        earlier = vector
        vector = residual / beta_now[:, None, None]
        beta_before = beta_now
        alpha_list.append(alpha_now)
        beta_list.append(beta_now)
    return (vector, earlier, jnp.stack(alpha_list, axis=1), jnp.stack(beta_list, axis=1))
```

```python
import functools

import jax
import jax.numpy as jnp
from jax import lax
from jax.experimental import pallas as pl
from jax.experimental.pallas import tpu as pltpu
from jax.sharding import PartitionSpec as P

STEPS = 3
LANES = 128

epsilon = 1e-06


def mark(name):
    pass


def partner(me, i, n):
    i = jnp.int32(i)
    out = jnp.int32(0)
    bit = 1
    while bit < n:
        out = out + lax.rem(lax.div(me, bit) + lax.div(i, bit), 2) * bit
        bit *= 2
    return out


def kernel(
    dims,
    energies_hbm, current_hbm, previous_hbm, beta_hbm, index_hbm,
    right_hbm, left_hbm, screened_hbm,
    result_ref,
    energies, current, previous, beta_in, index,
    right, left, screened, starts, packs, dens, held, fields, directs, sums,
    select, acc,
    small_sem, right_sem, left_sem, screened_sem,
    start_s, start_r, pack_s, pack_r, dens_s, line_r, chunk_r, field_s, field_r,
    direct_s, direct_r, sums_s, sums_r,
):
    nkp, npw, kl, nv, bands, gs = dims
    rows = kl * nv
    total = rows * nkp
    entries = total // nv * bands
    points = nkp * kl
    f32, bf16 = jnp.float32, jnp.bfloat16
    kme = lax.axis_index("kpt")
    pme = lax.axis_index("pw")

    def send(src, dst, i, j, ssem, rsem):
        device = {}
        if i:
            device["kpt"] = partner(kme, i, nkp)
        if j:
            device["pw"] = partner(pme, j, npw)
        pltpu.make_async_remote_copy(
            src_ref=src, dst_ref=dst, send_sem=ssem, recv_sem=rsem,
            device_id=device, device_id_type=pl.DeviceIdType.MESH,
        ).start()

    def bytes_of(ref, ssem, rsem):
        return pltpu.make_async_remote_copy(
            src_ref=ref, dst_ref=ref, send_sem=ssem, recv_sem=rsem,
            device_id={"pw": partner(pme, 1, npw)}, device_id_type=pl.DeviceIdType.MESH,
        )

    def arrived(ref, ssem, rsem):
        bytes_of(ref, ssem, rsem).wait_recv()

    pending = []

    small = [
        pltpu.make_async_copy(source, target, small_sem.at[n])
        for n, (source, target) in enumerate((
            (current_hbm, current), (previous_hbm, previous), (energies_hbm, energies),
            (beta_hbm, beta_in), (index_hbm, index),
        ))
    ]
    right_copy = pltpu.make_async_copy(right_hbm, right, right_sem)
    left_copy = pltpu.make_async_copy(left_hbm, left, left_sem)

    def screened_copy(j):
        first = pl.multiple_of(partner(pme, j, npw) * gs, gs)
        return pltpu.make_async_copy(
            screened_hbm.at[:, :, pl.ds(first, gs)], screened.at[j], screened_sem.at[j]
        )

    mark("start")
    for copy in small:
        copy.start()
    barrier = pltpu.get_barrier_semaphore()
    greet = [(0, j) for j in range(npw - 1, 0, -1)]
    greet += [(i, b) for i in range(nkp - 1, 0, -1) for b in range(2)]
    for i, j in greet:
        device = {"kpt": partner(kme, i, nkp), "pw": partner(pme, j, npw)}
        pl.semaphore_signal(
            barrier, inc=1, device_id=device, device_id_type=pl.DeviceIdType.MESH
        )
    right_copy.start()
    for j in range(npw):
        screened_copy(j).start()
    left_copy.start()

    width = energies.shape[1]
    per = LANES // width
    turn_at = lax.rem(pme, per)

    def spread_lanes(block):
        return jnp.concatenate(
            [block * (turn_at == j).astype(f32) for j in range(per)], axis=1
        )

    small[0].wait()
    own_current = jnp.concatenate([current[v] for v in range(nv)], axis=0)
    starts[0] = spread_lanes(own_current).astype(bf16)
    mark("barrier")
    pl.semaphore_wait(barrier, len(greet))
    mark("startsend")
    for j in range(npw - 1, 0, -1):
        send(starts.at[0], starts.at[j], 0, j, start_s, start_r)
    pending.append(bytes_of(starts.at[pl.ds(1, npw - 1)], start_s, start_r))
    small[1].wait()
    small[2].wait()
    own_levels = energies[...]
    packs[0] = spread_lanes(jnp.concatenate(
        [own_current] + [previous[v] for v in range(nv)] + [own_levels] * nv, axis=0
    ))
    for j in range(npw - 1, 0, -1):
        send(packs.at[0], packs.at[j], 0, j, pack_s, pack_r)
    pending.append(bytes_of(packs.at[pl.ds(1, npw - 1)], pack_s, pack_r))

    small[4].wait()
    wide = kl * total

    def points_of(shape):
        row = lax.rem(lax.broadcasted_iota(jnp.int32, shape, 0), total)
        base = jnp.zeros(shape, jnp.int32)
        for i in range(nkp):
            base = jnp.where(row // rows == i, partner(kme, i, nkp) * kl, base)
        col = lax.broadcasted_iota(jnp.int32, shape, 1)
        return (base + lax.rem(row, kl) == col).astype(bf16)

    table = index[...].astype(f32).astype(bf16)
    pairs = jnp.dot(points_of((total, points)), table, preferred_element_type=f32).astype(bf16)
    pairs = lax.dot_general(
        pairs, points_of((wide, points)), (((1,), (1,)), ((), ())), preferred_element_type=f32
    )
    col = lax.broadcasted_iota(jnp.int32, (total, wide), 1)
    row = lax.broadcasted_iota(jnp.int32, (total, wide), 0)
    transfer = (kme * kl + col // total).astype(f32)
    same = (lax.rem(row, rows) // kl == lax.rem(col, rows) // kl).astype(f32)
    pick = (same * jnp.maximum(1.0 - jnp.abs(pairs - transfer), 0.0)).astype(bf16)
    select[...] = jnp.concatenate([pick, pick], axis=1)

    row_g = lax.rem(lax.broadcasted_iota(jnp.int32, (rows, gs), 0), kl)
    row_c = lax.rem(lax.broadcasted_iota(jnp.int32, (rows, bands), 0), kl)
    row_v = lax.broadcasted_iota(jnp.int32, (rows, LANES), 0) // kl
    lane = lax.broadcasted_iota(jnp.int32, (rows, LANES), 1)

    def joined(buf, part):
        tiles = []
        for m in range(bands // LANES):
            slots = [buf[partner(pme, m * per + j, npw)].astype(f32) for j in range(per)]
            tiles.append(sum(slots))
        return jnp.concatenate(tiles, axis=1)

    def density(x, split):
        high = x.astype(bf16)
        both = high
        if split:
            high = high.astype(f32)
            both = jnp.concatenate([high, x - high], axis=0).astype(bf16)
        out = jnp.zeros((rows, gs), f32)
        for k in range(kl):
            res = jnp.dot(both, right[k], preferred_element_type=f32)
            if split:
                res = res[:rows] + res[rows:]
            out = jnp.where(row_g == k, res, out)
        return out.astype(bf16)

    def tile_of(columns):
        tile = jnp.zeros((rows, LANES), f32)
        for n, column in enumerate(columns):
            tile = jnp.where(lane == n, jnp.sum(column, axis=1, keepdims=True), tile)
        return tile

    def share_sums(step, columns):
        buf = sums.at[step]
        buf[0] = tile_of(columns)
        for i in range(nkp - 1, 0, -1):
            send(buf.at[0], buf.at[i], i, 0, sums_s.at[step], sums_r.at[step])
        pending.append(bytes_of(buf.at[pl.ds(1, nkp - 1)], sums_s.at[step], sums_r.at[step]))

    def take_sums(step, count):
        buf = sums.at[step]
        arrived(buf.at[pl.ds(1, nkp - 1)], sums_s.at[step], sums_r.at[step])
        tile = sum(buf[partner(kme, s, nkp)] for s in range(nkp))
        out = jnp.zeros_like(tile)
        for v in range(nv):
            chain = jnp.sum(jnp.where(row_v == v, tile, 0.0), axis=0, keepdims=True)
            out = jnp.where(row_v == v, chain, out)
        return [out[:, n : n + 1] * (1.0 / entries) for n in range(count)]

    def scalars(uv, uu, vv, sigma):
        gamma = uv + sigma * (vv - 1.0)
        beta = jnp.sqrt(uu - 2.0 * gamma * uv + gamma * gamma * vv + epsilon)
        return gamma, beta

    coef = jnp.zeros((rows, LANES), f32)
    mark("startwait")
    arrived(starts.at[pl.ds(1, npw - 1)], start_s, start_r)
    mark("rightwait")
    right_copy.wait()
    x = joined(starts, rows)
    vec = early = levels = base = image = sigma = unit = None
    for turn in range(STEPS):
        mark(f"dens{turn}")
        gather = dens.at[turn]
        gather[0] = density(x, turn > 0)
        gsend = dens_s.at[turn]
        for j in range(npw - 2, 0, -2):
            send(gather.at[0], gather.at[j * nkp], 0, j, gsend, line_r.at[turn, j // 2])
        for i in range(nkp - 1, 0, -1):
            for b in range(2):
                send(gather.at[0], gather.at[b * nkp + i], i, b, gsend, chunk_r.at[turn, b])
        send(gather.at[0], gather.at[nkp], 0, 1, gsend, chunk_r.at[turn, 1])
        pending.append(bytes_of(gather.at[pl.ds(1, npw * nkp - 1)], gsend, chunk_r.at[turn, 0]))
        if turn > 0:
            mark(f"sums{turn}")
            share_sums(turn, [
                x * vec, x * x, vec * vec, levels * x * x, levels * x * vec, levels * vec * vec
            ])
        mark(f"relay{turn}")
        for j in range(2, npw, 2):
            arrived(gather.at[j * nkp], gsend, line_r.at[turn, j // 2])
            for i in range(nkp - 1, 0, -1):
                for b in range(2):
                    send(
                        gather.at[j * nkp], gather.at[(j + b) * nkp + i], i, b,
                        gsend, chunk_r.at[turn, j + b],
                    )
            send(gather.at[j * nkp], gather.at[(j + 1) * nkp], 0, 1, gsend, chunk_r.at[turn, j + 1])
        if turn == 0:
            mark("packwait")
            arrived(packs.at[pl.ds(1, npw - 1)], pack_s, pack_r)
            whole = joined(packs, 3 * rows)
            vec = whole[:rows]
            early = whole[rows : 2 * rows]
            levels = whole[2 * rows :]
            share_sums(0, [levels * vec * vec, vec * early])
        for j in range(0, npw, 2):
            mark(f"chunkwait{turn}_{j}")
            arrived(gather.at[pl.ds(j * nkp + 1, nkp - 1)], gsend, chunk_r.at[turn, j])
            arrived(gather.at[pl.ds((j + 1) * nkp, nkp)], gsend, chunk_r.at[turn, j + 1])
            if turn == 0:
                screened_copy(j).wait()
                screened_copy(j + 1).wait()
            mark(f"prod{turn}_{j}")
            left_sides = [
                gather[(j + b) * nkp : (j + b + 1) * nkp].reshape(total, gs) for b in range(2)
            ]
            for q in range(kl):
                part = sum(
                    lax.dot_general(
                        left_sides[b], screened[j + b, q],
                        (((1,), (1,)), ((), ())), preferred_element_type=f32,
                    )
                    for b in range(2)
                )
                if j:
                    part = part + acc[q * total : (q + 1) * total]
                acc[q * total : (q + 1) * total] = part
        mark(f"select{turn}")
        images = acc[...]
        high = images.astype(bf16)
        low = (images - high.astype(f32)).astype(bf16)
        out = jnp.dot(
            select[...], jnp.concatenate([high, low], axis=0), preferred_element_type=f32
        )
        for i in range(nkp - 1, 0, -1):
            held[turn, i] = out[i * rows : (i + 1) * rows].astype(bf16)
            send(
                held.at[turn, i], fields.at[turn, i], i, 0, field_s.at[turn], field_r.at[turn]
            )
        pending.append(
            bytes_of(held.at[turn, pl.ds(1, nkp - 1)], field_s.at[turn], field_r.at[turn])
        )
        mark(f"scalars{turn}")
        if turn == 0:
            small[3].wait()
            first_beta = jnp.zeros((rows, 1), f32)
            for v in range(nv):
                first_beta = jnp.where(row_v[:, :1] == v, beta_in[0:1, v : v + 1], first_beta)
            evv, ve = take_sums(0, 2)
            sigma = evv - first_beta * ve
            base = levels * vec - first_beta * early - sigma * vec
            unit = None
            left_copy.wait()
        else:
            uv, uu, vv, euu, euv, evv = take_sums(turn, 6)
            gamma, beta = scalars(uv, uu, vv, sigma)
            coef = jnp.where(lane == turn - 1, gamma + sigma, coef)
            coef = jnp.where(lane == STEPS + turn - 1, beta, coef)
            unit = 1.0 / beta
            sigma = (euu - 2.0 * gamma * euv + gamma * gamma * evv) * unit * unit - (uv - gamma * vv)
            early = vec
            vec = (x - gamma * vec) * unit
            ratio = gamma * unit
            base = levels * vec - beta * early - sigma * vec + ratio * image
        mark(f"fieldwait{turn}")
        arrived(fields.at[turn, pl.ds(1, nkp - 1)], field_s.at[turn], field_r.at[turn])
        mark(f"left{turn}")
        field = out[:rows]
        for i in range(1, nkp):
            field = field + fields[turn, i].astype(f32)
        field = field.astype(bf16)
        part = jnp.zeros((rows, bands), f32)
        for k in range(kl):
            res = lax.dot_general(
                field, left[k], (((1,), (1,)), ((), ())), preferred_element_type=f32
            )
            part = jnp.where(row_c == k, res, part)
        shared = directs.at[turn]
        shared[0] = part.astype(bf16)
        for j in range(npw - 1, 0, -1):
            send(shared.at[0], shared.at[j], 0, j, direct_s.at[turn], direct_r.at[turn])
        pending.append(
            bytes_of(shared.at[pl.ds(1, npw - 1)], direct_s.at[turn], direct_r.at[turn])
        )
        mark(f"dirwait{turn}")
        arrived(shared.at[pl.ds(1, npw - 1)], direct_s.at[turn], direct_r.at[turn])
        mark(f"applied{turn}")
        direct = sum(shared[partner(pme, s, npw)].astype(f32) for s in range(npw))
        if turn == 0:
            image = direct
            x = base - direct
        else:
            image = direct * unit - ratio * image
            x = base - direct * unit
    mark("final")
    share_sums(STEPS, [x * vec, x * x, vec * vec])
    owns = []
    for source in (x, vec):
        own = jnp.zeros((rows, width), f32)
        for m in range(npw):
            own = jnp.where(pme == m, source[:, m * width : (m + 1) * width], own)
        owns.append(own)
    mark("finalwait")
    uv, uu, vv = take_sums(STEPS, 3)
    mark("finalout")
    gamma, beta = scalars(uv, uu, vv, sigma)
    coef = jnp.where(lane == STEPS - 1, gamma + sigma, coef)
    coef = jnp.where(lane == 2 * STEPS - 1, beta, coef)
    result_ref[0, :, :width] = (owns[0] - gamma * owns[1]) / beta
    result_ref[1, :, :width] = owns[1]
    result_ref[2] = coef
    mark("pending")
    for copy in pending:
        copy.wait_send()
    mark(None)


def unpack(result_ref, last_ref, prior_ref, alphas_ref, betas_ref):
    nv, kl, width = last_ref.shape
    for v in range(nv):
        last_ref[v] = result_ref[0, v * kl : (v + 1) * kl, :width]
        prior_ref[v] = result_ref[1, v * kl : (v + 1) * kl, :width]
        alphas_ref[v : v + 1, :] = result_ref[2, v * kl : v * kl + 1, :STEPS]
        betas_ref[v : v + 1, :] = result_ref[2, v * kl : v * kl + 1, STEPS : 2 * STEPS]


def on_device(
    nkp, npw,
    energies, current, previous, previous_beta, pair_left, pair_right, screened, momentum_index
):
    nv, kl, width = current.shape
    bands = pair_left.shape[1]
    gs = pair_left.shape[2]
    qcount = screened.shape[0]
    rows = kl * nv
    total = rows * nkp
    f32, bf16 = jnp.float32, jnp.bfloat16
    vmem = pl.BlockSpec(memory_space=pltpu.VMEM)
    hbm = pl.BlockSpec(memory_space=pltpu.HBM)
    dma = pltpu.SemaphoreType.DMA
    result = pl.pallas_call(
        functools.partial(kernel, (nkp, npw, kl, nv, bands, gs)),
        out_shape=jax.ShapeDtypeStruct((3, rows, LANES), f32),
        in_specs=[hbm] * 8,
        out_specs=vmem,
        scratch_shapes=[
            pltpu.VMEM(energies.shape, f32),
            pltpu.VMEM(current.shape, f32),
            pltpu.VMEM(current.shape, f32),
            pltpu.VMEM((1, nv), f32),
            pltpu.VMEM(momentum_index.shape, jnp.int32),
            pltpu.VMEM((kl, bands, gs), bf16),
            pltpu.VMEM((kl, bands, gs), bf16),
            pltpu.VMEM((npw, qcount, gs, gs), bf16),
            pltpu.VMEM((npw, rows, LANES), bf16),
            pltpu.VMEM((npw, 3 * rows, LANES), f32),
            pltpu.VMEM((STEPS, npw * nkp, rows, gs), bf16),
            pltpu.VMEM((STEPS, nkp, rows, gs), bf16),
            pltpu.VMEM((STEPS, nkp, rows, gs), bf16),
            pltpu.VMEM((STEPS, npw, rows, bands), bf16),
            pltpu.VMEM((STEPS + 1, nkp, rows, LANES), f32),
            pltpu.VMEM((total, 2 * qcount * total), bf16),
            pltpu.VMEM((qcount * total, gs), f32),
            dma((5,)), dma, dma, dma((npw,)),
            dma, dma, dma, dma,
            dma((STEPS,)), dma((STEPS, npw // 2)), dma((STEPS, npw)),
            dma((STEPS,)), dma((STEPS,)),
            dma((STEPS,)), dma((STEPS,)),
            dma((STEPS + 1,)), dma((STEPS + 1,)),
        ],
        compiler_params=pltpu.CompilerParams(
            collective_id=0, has_side_effects=True, vmem_limit_bytes=60 * 1024 * 1024
        ),
    )(
        energies, current, previous, previous_beta[None], momentum_index,
        pair_right, pair_left, screened,
    )
    return pl.pallas_call(
        unpack,
        out_shape=(
            jax.ShapeDtypeStruct(current.shape, f32),
            jax.ShapeDtypeStruct(current.shape, f32),
            jax.ShapeDtypeStruct((nv, STEPS), f32),
            jax.ShapeDtypeStruct((nv, STEPS), f32),
        ),
        in_specs=[vmem],
        out_specs=(vmem, vmem, vmem, vmem),
    )(result)


def solution(mesh):
    return jax.shard_map(
        functools.partial(on_device, mesh.shape["kpt"], mesh.shape["pw"]),
        mesh=mesh,
        in_specs=(
            P("kpt", "pw"),
            P(None, "kpt", "pw"),
            P(None, "kpt", "pw"),
            P(),
            P("kpt", None, "pw"),
            P("kpt", None, "pw"),
            P("kpt", "pw", None),
            P(),
        ),
        out_specs=(P(None, "kpt", "pw"), P(None, "kpt", "pw"), P(), P()),
        check_vma=False,
    )
```
